32 devices in a mesh: dp: 8 (over z, x), tensor: 4 (over y, core).
Axes of the slice: x: 2, y: 2, z: 4, core: 2. Of those that a mesh axis runs over, the one named last changes fastest.
Arguments:
- tokens: bfloat16 [4096, 4608], P(('dp', 'tensor')), parts along dimension 0, may hold values from -6 to 6
- pre_gain: float32 [4608], replicated, may hold values from 0.1 to 1.9
- query_weight: bfloat16 [4608, 4096], P(None, 'tensor'), as said below
- key_weight: bfloat16 [4608, 2048], P(None, 'tensor'), as said below
- value_weight: bfloat16 [4608, 2048], P(None, 'tensor'), may hold values from -0.09375 to 0.09375
- out_weight: bfloat16 [4096, 4608], P('tensor'), may hold values from -0.09375 to 0.09375
- post_gain: float32 [4608], replicated, may hold values from 0.1 to 1.9
Outputs:
- layer_out: bfloat16 [4096, 4608], P(('dp', 'tensor')), parts along dimension 0
The draws below stay inside these ranges and needn't reach their ends.
There are 8 independent parts, one for each index of `dp`. The reference program is written for one: setup_inputs(seed, part) draws one part's arguments, and reference() takes and returns one part's arrays. A program takes and returns all parts, laid end to end along the dimension named above; an argument that names none is the same for every part. Nothing has to cross between parts.
Inputs may be any that keep to these rules, and one draw needn't show every extreme that they name: `query_weight`: entries lie within 16 / sqrt(4608) of zero. `key_weight`: entries lie within 16 / sqrt(4608) of zero.
All inputs are finite; a program needn't handle non-finite values.
Results may differ from the reference program's by a relative error of at most 0.015.
Values may be sent and summed in bfloat16 or wider, within the bound.
A program may use at most 192 MiB of HBM per device.

```python
import jax
import jax.numpy as jnp
from jax import lax

D = 4608
HEADS = 32
KV_HEADS = 16
HEAD_DIM = 128
SEQ_LEN = 128
SEQS = 4
TOKENS = 512
N_TENSOR = 4


def strong_head(key):
    return jax.random.randint(jax.random.fold_in(key, 5), (), 0, HEADS)


def head_gains(key, count, forced):
    spread = jax.random.uniform(key, (count,), jnp.float32)
    spread = jnp.where(jnp.arange(count) == forced, 1.0, spread)
    return 0.5 * jnp.power(8.0, spread)


def scaled_weight(key, count, forced):
    gains = head_gains(jax.random.fold_in(key, 1), count, forced)
    entries = jnp.clip(jax.random.normal(jax.random.fold_in(key, 2), (D, count * HEAD_DIM), jnp.float32), -4.0, 4.0)
    column_gain = jnp.repeat(gains, HEAD_DIM)
    return (entries * column_gain[None, :] / jnp.sqrt(jnp.float32(D))).astype(jnp.bfloat16)


def draw_query_weight(key, part):
    forced = strong_head(key)
    return scaled_weight(jax.random.fold_in(key, 11), HEADS, forced)


def draw_key_weight(key, part):
    forced = strong_head(key) // (HEADS // KV_HEADS)
    return scaled_weight(jax.random.fold_in(key, 23), KV_HEADS, forced)


def levels(rng, extent, shards, low, high):
    gain = 1.0
    for axis_at, blocks in shards:
        draws = jax.random.uniform(jax.random.fold_in(jax.random.fold_in(rng, 6), axis_at), (blocks,), jnp.float32, low / len(shards), high / len(shards))
        gain = gain * jnp.repeat(jnp.exp(draws), extent[axis_at] // blocks).reshape((-1,) + (1,) * (len(extent) - 1 - axis_at))
    return gain


def scatter_about(stream_key, shape, scale, reach, shards=(), kind=jnp.bfloat16):
    level = levels(stream_key, shape, shards, -0.22, 0.18) if shards else 1.0
    result = jax.random.normal(stream_key, shape, jnp.float32) * scale * level
    return jnp.minimum(jnp.maximum(result, -reach), reach).astype(kind)


def setup_inputs(seed: int = 0, part: int = 0) -> dict:
    key_list = jax.random.split(jax.random.key(seed), 8)
    own_keys = jax.random.split(jax.random.fold_in(key_list[7], part), 8)
    tokens = scatter_about(own_keys[0], (TOKENS, D), 1.0, 6.0, ((0, 4),))
    pre_gain = jnp.clip(1.0 + 0.18 * jax.random.normal(key_list[1], (D,), jnp.float32), 0.1, 1.9)
    query_weight = draw_query_weight(jax.random.fold_in(key_list[7], 71), part)
    key_weight = draw_key_weight(jax.random.fold_in(key_list[7], 71), part)
    value_weight = scatter_about(key_list[4], (D, KV_HEADS * HEAD_DIM), D ** -0.5, 0.09375, ((1, 4),))
    out_weight = scatter_about(key_list[5], (HEADS * HEAD_DIM, D), (HEADS * HEAD_DIM) ** -0.5, 0.09375, ((0, 4),))
    post_gain = jnp.clip(1.0 + 0.18 * jax.random.normal(key_list[6], (D,), jnp.float32), 0.1, 1.9)
    return dict(tokens=tokens, pre_gain=pre_gain, query_weight=query_weight, key_weight=key_weight, value_weight=value_weight, out_weight=out_weight, post_gain=post_gain)


norm_epsilon = 1e-06
soft_cap = 50.0
query_scale = 1.0 / 12.0
rope_base = 10000.0

def rms_scale(vectors, scale_gain):
    mean_square = lax.optimization_barrier(jnp.mean(vectors * vectors, axis=-1, keepdims=True))
    return vectors * lax.rsqrt(mean_square + norm_epsilon) * scale_gain.astype(jnp.float32)

def rotate(vectors, positions):
    half_dim = vectors.shape[-1] // 2
    exponent = jnp.arange(half_dim, dtype=jnp.float32) / half_dim
    angles = positions.astype(jnp.float32)[:, None] * jnp.power(rope_base, -exponent)[None, :]
    cosine = jnp.cos(angles)[:, None, :]
    sine_part = jnp.sin(angles)[:, None, :]
    first_half = vectors[..., :half_dim]
    second_half = vectors[..., half_dim:]
    return jnp.concatenate([first_half * cosine - second_half * sine_part, second_half * cosine + first_half * sine_part], axis=-1)

def attend(query, keys, values, query_pos, key_pos):
    query_count = query.shape[0]
    key_count = keys.shape[0]
    key_heads = keys.shape[1] // HEAD_DIM
    groups = query.shape[1] // keys.shape[1]
    query_four = query.reshape(query_count, key_heads, groups, HEAD_DIM).astype(jnp.float32)
    key_three = keys.reshape(key_count, key_heads, HEAD_DIM).astype(jnp.float32)
    value_three = values.reshape(key_count, key_heads, HEAD_DIM).astype(jnp.float32)
    raw_scores = jnp.einsum('qhgd,khd->hgqk', query_four, key_three, precision=lax.Precision.HIGHEST)
    capped = soft_cap * jnp.tanh(raw_scores * query_scale / soft_cap)
    allowed = jnp.logical_and(key_pos[None, :] <= query_pos[:, None], key_pos[None, :] // SEQ_LEN == query_pos[:, None] // SEQ_LEN)
    weights = jnp.where(allowed[None, None], jnp.exp(capped), 0.0)
    probability = (weights / lax.optimization_barrier(jnp.sum(weights, axis=-1, keepdims=True))).astype(jnp.bfloat16)
    mixed = jnp.einsum('hgqk,khd->qhgd', probability.astype(jnp.float32), value_three, precision=lax.Precision.HIGHEST)
    return mixed.astype(jnp.bfloat16).reshape(query_count, -1)

def reference(tokens, pre_gain, query_weight, key_weight, value_weight, out_weight, post_gain):
    token_count = tokens.shape[0]
    normed = rms_scale(tokens.astype(jnp.float32), pre_gain).astype(jnp.bfloat16)
    positions = jnp.arange(token_count, dtype=jnp.int32) % SEQ_LEN
    query = jnp.dot(normed, query_weight, preferred_element_type=jnp.float32)
    keys = jnp.dot(normed, key_weight, preferred_element_type=jnp.float32)
    values = jnp.dot(normed, value_weight, preferred_element_type=jnp.float32).astype(jnp.bfloat16)
    query = rotate(query.reshape(token_count, HEADS, HEAD_DIM), positions).reshape(token_count, HEADS * HEAD_DIM).astype(jnp.bfloat16)
    keys = rotate(keys.reshape(token_count, KV_HEADS, HEAD_DIM), positions).reshape(token_count, KV_HEADS * HEAD_DIM).astype(jnp.bfloat16)

    def one_sequence(seq_index):
        first_row = (seq_index * SEQ_LEN).astype(jnp.int32)
        token_pos = first_row + jnp.arange(SEQ_LEN, dtype=jnp.int32)
        return attend(lax.dynamic_slice_in_dim(query, first_row, SEQ_LEN, 0), lax.dynamic_slice_in_dim(keys, first_row, SEQ_LEN, 0), lax.dynamic_slice_in_dim(values, first_row, SEQ_LEN, 0), token_pos, token_pos)
    attended = lax.map(one_sequence, jnp.arange(SEQS, dtype=jnp.int32)).reshape(token_count, HEADS * HEAD_DIM)
    group_cols = HEADS * HEAD_DIM // N_TENSOR

    def add_group(group_index, running):
        first_col = (group_index * group_cols).astype(jnp.int32)
        group_term = jnp.dot(lax.dynamic_slice_in_dim(attended, first_col, group_cols, 1), lax.dynamic_slice_in_dim(out_weight, first_col, group_cols, 0), preferred_element_type=jnp.float32)
        rounded = lax.optimization_barrier(group_term.astype(jnp.bfloat16))
        return running + rounded.astype(jnp.float32)
    mixed = lax.fori_loop(0, N_TENSOR, add_group, jnp.zeros((token_count, D), jnp.float32))
    branch = rms_scale(mixed, post_gain)
    return (tokens.astype(jnp.float32) + branch).astype(jnp.bfloat16)
```

```python
import functools

import jax
import jax.numpy as jnp
import numpy as np
from jax import lax
from jax.experimental import pallas as pl
from jax.experimental.pallas import tpu as pltpu
from jax.sharding import PartitionSpec as P

HEAD_DIM = 128
SEQ_LEN = 128


norm_epsilon = 1e-06
soft_cap = 50.0
query_scale = 1.0 / 12.0
rope_base = 10000.0


def rms_scale(vectors, scale_gain):
    mean_square = jnp.mean(vectors * vectors, axis=-1, keepdims=True)
    return vectors * lax.rsqrt(mean_square + norm_epsilon) * scale_gain


def rotate(vectors, positions):
    half_dim = vectors.shape[-1] // 2
    exponent = jnp.arange(half_dim, dtype=jnp.float32) / half_dim
    angles = positions.astype(jnp.float32)[:, None] * jnp.power(rope_base, -exponent)[None, :]
    cosine = jnp.cos(angles)[:, None, :]
    sine_part = jnp.sin(angles)[:, None, :]
    first_half = vectors[..., :half_dim]
    second_half = vectors[..., half_dim:]
    return jnp.concatenate(
        [
            first_half * cosine - second_half * sine_part,
            second_half * cosine + first_half * sine_part,
        ],
        axis=-1,
    )


def project_block(normed, query_weight, key_weight, value_weight):
    block_rows = normed.shape[0]
    positions = jnp.arange(block_rows, dtype=jnp.int32) % SEQ_LEN
    query = jnp.dot(normed, query_weight, preferred_element_type=jnp.float32)
    keys = jnp.dot(normed, key_weight, preferred_element_type=jnp.float32)
    values = jnp.dot(normed, value_weight, preferred_element_type=jnp.float32)
    query = rotate(query.reshape(block_rows, -1, HEAD_DIM), positions).reshape(block_rows, -1)
    keys = rotate(keys.reshape(block_rows, -1, HEAD_DIM), positions).reshape(block_rows, -1)
    return jnp.concatenate(
        [query.astype(jnp.bfloat16), keys.astype(jnp.bfloat16), values.astype(jnp.bfloat16)], axis=1
    )


def attend(query, keys, values, query_pos, key_pos):
    query_count = query.shape[0]
    key_count = keys.shape[0]
    key_heads = keys.shape[1] // HEAD_DIM
    groups = query.shape[1] // keys.shape[1]
    query_four = query.reshape(query_count, key_heads, groups, HEAD_DIM)
    key_three = keys.reshape(key_count, key_heads, HEAD_DIM)
    value_three = values.reshape(key_count, key_heads, HEAD_DIM)
    raw_scores = jnp.einsum(
        "qhgd,khd->hgqk", query_four, key_three, preferred_element_type=jnp.float32
    )
    capped = soft_cap * jnp.tanh(raw_scores * query_scale / soft_cap)
    allowed = jnp.logical_and(
        key_pos[None, :] <= query_pos[:, None],
        key_pos[None, :] // SEQ_LEN == query_pos[:, None] // SEQ_LEN,
    )
    weights = jnp.where(allowed[None, None], jnp.exp(capped), 0.0)
    probability = (weights / jnp.sum(weights, axis=-1, keepdims=True)).astype(jnp.bfloat16)
    mixed = jnp.einsum(
        "hgqk,khd->qhgd", probability, value_three, preferred_element_type=jnp.float32
    )
    return mixed.astype(jnp.bfloat16).reshape(query_count, -1)


def staged(tokens, pre_gain, query_weight, key_weight, value_weight, out_weight, post_gain):
    local_rows = tokens.shape[0]
    query_cols = query_weight.shape[1]
    key_cols = key_weight.shape[1]
    normed = rms_scale(tokens.astype(jnp.float32), pre_gain).astype(jnp.bfloat16)
    stacked = project_block(
        lax.all_gather(normed, "tensor", axis=0, tiled=True), query_weight, key_weight, value_weight
    )
    query = stacked[:, :query_cols]
    keys = stacked[:, query_cols : query_cols + key_cols]
    values = stacked[:, query_cols + key_cols :]
    token_count = stacked.shape[0]
    key_count = min(token_count, lax.axis_size("tensor") * local_rows + SEQ_LEN)
    key_first = jnp.clip(jnp.int32(0) // SEQ_LEN * SEQ_LEN, 0, token_count - key_count)
    query_pos = jnp.arange(lax.axis_size("tensor") * local_rows, dtype=jnp.int32)
    key_pos = key_first + jnp.arange(key_count, dtype=jnp.int32)
    block_out = attend(query, keys, values, query_pos, key_pos)
    mixed = lax.psum_scatter(
        jnp.dot(block_out, out_weight, preferred_element_type=jnp.float32).astype(jnp.bfloat16),
        "tensor",
        scatter_dimension=0,
        tiled=True,
    ).astype(jnp.float32)
    branch = rms_scale(mixed, post_gain)
    return (tokens.astype(jnp.float32) + branch).astype(jnp.bfloat16)


def rope_tables():
    half_dim = HEAD_DIM // 2
    angles = np.arange(SEQ_LEN)[:, None] * np.power(rope_base, -np.arange(half_dim) / half_dim)[None, :]
    cosine, sine = np.cos(angles), np.sin(angles)
    return np.stack(
        [np.concatenate([cosine, cosine], 1), np.concatenate([-sine, sine], 1)]
    ).astype(np.float32)


def divisor(count, wanted):
    return next(k for k in range(min(wanted, count), 0, -1) if count % k == 0)


def copy_to(src, dst, send_sem, recv_sem, index):
    return pltpu.make_async_remote_copy(
        src_ref=src,
        dst_ref=dst,
        send_sem=send_sem,
        recv_sem=recv_sem,
        device_id={"tensor": index},
        device_id_type=pl.DeviceIdType.MESH,
    )


def fused_kernel(
    cuts,
    row_cuts,
    head_rows,
    keep_rows,
    tokens,
    pre_gain,
    query_weight,
    key_weight,
    value_weight,
    out_weight,
    post_gain,
    rope_table,
    out,
    xbuf,
    scaled,
    acc,
    square,
    weight,
    out_half,
    attended,
    part,
    local_in,
    remote_in,
    gain_pre,
    gain_post,
    rope,
    in_sem,
    w_sem,
    wo_sem,
    x_send,
    x_recv,
    link_send,
    link_recv,
    fwd_send,
    fwd_recv,
    att_send,
    att_recv,
    lp_send,
    lp_recv,
    rp_send,
    rp_recv,
):
    rows, width = tokens.shape
    q_cols = query_weight.shape[1]
    k_cols = key_weight.shape[1]
    all_cols = q_cols + 2 * k_cols
    half = width // 2
    chunk = half // cuts
    groups = q_cols // k_cols
    kv_heads = k_cols // HEAD_DIM
    step_rows = rows // row_cuts
    n_tile = all_cols // divisor(all_cols // 128, 4)
    o_tile = half // divisor(half // 128, 3)

    me = lax.axis_index("tensor")
    core = me % 2
    other = 1 - core
    side = me // 2
    mate = side * 2 + other
    far = (1 - side) * 2

    def cols(start, size):
        return pl.ds(pl.multiple_of(start, 128), size)

    def rws(start, size):
        return pl.ds(pl.multiple_of(start, 16), size)

    def landed(ref, sem):
        copy_to(ref, ref, sem, sem, mate).wait_recv()

    def left(ref, sem):
        copy_to(ref, ref, sem, sem, mate).wait_send()

    own = pltpu.make_async_copy(tokens, xbuf.at[rws(core * rows, rows)], in_sem.at[0])
    own.start()
    small = [
        pltpu.make_async_copy(pre_gain, gain_pre, in_sem.at[1]),
        pltpu.make_async_copy(post_gain, gain_post, in_sem.at[2]),
        pltpu.make_async_copy(rope_table, rope, in_sem.at[3]),
    ]

    def weight_rows(k):
        return pl.ds(pl.multiple_of(k * chunk, 128), chunk)

    def weight_start(k):
        at = weight_rows(k)
        sem = w_sem.at[k]
        pltpu.make_async_copy(query_weight.at[at], weight.at[at, 0:q_cols], sem).start()
        pltpu.make_async_copy(key_weight.at[at], weight.at[at, q_cols : q_cols + k_cols], sem).start()
        pltpu.make_async_copy(value_weight.at[at], weight.at[at, q_cols + k_cols : all_cols], sem).start()

    def weight_wait(k):
        ref = weight.at[weight_rows(k)]
        pltpu.make_async_copy(ref, ref, w_sem.at[k]).wait()

    barrier = pltpu.get_barrier_semaphore()
    for index in (mate, far, far + 1):
        pl.semaphore_signal(
            barrier, inc=1, device_id={"tensor": index}, device_id_type=pl.DeviceIdType.MESH
        )
    pl.semaphore_wait(barrier, 3)

    def x_copy(owner, h, sem):
        ref = xbuf.at[rws(owner * rows, rows), cols(h * half, half)]
        return copy_to(ref, ref, x_send.at[0], x_recv.at[sem], mate)

    def far_chunk(s, j, h):
        return xbuf.at[pl.ds((2 + s) * rows, rows), cols(h * half + j * chunk, chunk)]

    def link_at(s, j, h, first, last, sem, source=None):
        at = cols(h * half + j * chunk, chunk)
        if source is None:
            source = xbuf.at[pl.ds(s * rows + first, last - first), at]
        return copy_to(
            source,
            xbuf.at[pl.ds((2 + s) * rows + first, last - first), at],
            link_send.at[sem],
            link_recv.at[s, j],
            far + h,
        )

    def link_copy(s, j):
        first = head_rows if j == 0 else 0
        if s == 1 and j == cuts - 1:
            return link_at(s, j, core, first, keep_rows, 2)
        return link_at(s, j, core, first, rows, s)

    def head_copy(s, source=None):
        return link_at(s, 0, core, 0, head_rows, s, source)

    def tail_copy(h):
        return link_at(1, cuts - 1, h, keep_rows, rows, 3)

    @pl.when(core == 0)
    def _():
        head_copy(0, tokens.at[0:head_rows, cols(core * half, chunk)]).start()

    @pl.when(core == 1)
    def _():
        head_copy(1, tokens.at[0:head_rows, cols(core * half, chunk)]).start()

    for copy in small:
        copy.start()
    own.wait()
    x_copy(core, other, 0).start()

    @pl.when(core == 0)
    def _():
        for j in range(cuts):
            link_copy(0, j).start()

    x_copy(core, core, 1).start()

    def start_weights(k, _):
        weight_start(k)
        return 0

    lax.fori_loop(0, 2 * cuts, start_weights, 0)

    x_copy(other, core, 0).wait_recv()

    @pl.when(core == 1)
    def _():
        head_copy(0).start()
        for j in range(cuts):
            link_copy(0, j).start()
        for j in range(cuts - 1):
            link_copy(1, j).start()
        tail_copy(0).start()
        link_copy(1, cuts - 1).start()
        tail_copy(1).start()

    @pl.when(core == 0)
    def _():
        head_copy(1).start()
        for j in range(cuts):
            link_copy(1, j).start()

    own_out = pltpu.make_async_copy(
        out_weight.at[:, cols(core * half, half)],
        out_half.at[rws(core * q_cols, q_cols)],
        in_sem.at[0],
    )
    own_out.start()
    push_out = copy_to(
        out_weight.at[:, cols(other * half, half)],
        out_half.at[rws(core * q_cols, q_cols)],
        wo_sem.at[0],
        wo_sem.at[1],
        mate,
    )
    push_out.start()
    x_copy(other, other, 1).wait_recv()
    for copy in small:
        copy.wait()

    def project(first_row, acc_row, count, k):
        ar = pl.ds(acc_row, count)
        at = cols(k * chunk, chunk)
        total = square[ar]
        for i in range(chunk // 128):
            x = xbuf[pl.ds(first_row, count), cols(k * chunk + i * 128, 128)].astype(jnp.float32)
            total = total + x * x
            gain = gain_pre[pl.ds(k * (chunk // 128) + i, 1)]
            scaled[0:count, i * 128 : (i + 1) * 128] = (x * gain).astype(jnp.bfloat16)
        square[ar] = total

        def tile(n, _):
            nat = cols(n * n_tile, n_tile)
            acc[ar, nat] += jnp.dot(
                scaled[0:count], weight[at, nat], preferred_element_type=jnp.float32
            )
            return 0

        lax.fori_loop(0, all_cols // n_tile, tile, 0, unroll=True)

    def clear(row, count):
        acc[pl.ds(row, count)] = jnp.zeros((count, all_cols), jnp.float32)
        square[pl.ds(row, count)] = jnp.zeros((count, 128), jnp.float32)

    def attend_slot(acc_row, slot):
        ar = rws(acc_row, rows)
        scale = lax.rsqrt(
            jnp.sum(square[ar], axis=-1, keepdims=True) / width + norm_epsilon
        )
        cosine, sine = rope[0], rope[1]
        ok = lax.broadcasted_iota(jnp.int32, (rows, rows), 1) <= lax.broadcasted_iota(
            jnp.int32, (rows, rows), 0
        )
        ok = jnp.concatenate([ok] * groups, axis=0)

        def turned(at):
            v = acc[ar, at] * scale
            return (v * cosine + pltpu.roll(v, HEAD_DIM // 2, 1) * sine).astype(jnp.bfloat16)

        def head(g, _):
            query = jnp.concatenate(
                [turned(cols((g * groups + i) * HEAD_DIM, HEAD_DIM)) for i in range(groups)], axis=0
            )
            keys = turned(cols(q_cols + g * HEAD_DIM, HEAD_DIM))
            values = (acc[ar, cols(q_cols + k_cols + g * HEAD_DIM, HEAD_DIM)] * scale).astype(jnp.bfloat16)
            raw = lax.dot_general(
                query, keys, (((1,), (1,)), ((), ())), preferred_element_type=jnp.float32
            )
            capped = soft_cap * jnp.tanh(raw * (query_scale / soft_cap))
            mass = jnp.where(ok, jnp.exp(capped), 0.0)
            prob = (mass / jnp.sum(mass, axis=-1, keepdims=True)).astype(jnp.bfloat16)
            mixed = jnp.dot(prob, values, preferred_element_type=jnp.float32).astype(jnp.bfloat16)
            for i in range(groups):
                attended[
                    rws(slot * rows, rows), cols(core * q_cols + (g * groups + i) * HEAD_DIM, HEAD_DIM)
                ] = mixed[i * rows : (i + 1) * rows]
            return 0

        lax.fori_loop(0, kv_heads, head, 0)

    def att_copy(slot, whose):
        ref = attended.at[pl.ds(slot * rows, rows), cols(whose * q_cols, q_cols)]
        return copy_to(ref, ref, att_send.at[0], att_recv.at[max(slot - 1, 0)], mate)

    def out_project(slot):
        def tile(n, _):
            at = cols(n * o_tile, o_tile)
            part[rws(slot * rows, rows), at] = jnp.dot(
                attended[rws(slot * rows, rows)], out_half[:, at], preferred_element_type=jnp.float32
            ).astype(jnp.bfloat16)
            return 0

        lax.fori_loop(0, half // o_tile, tile, 0, unroll=True)

    clear(0, 3 * rows)

    def local_step(k, _):
        weight_wait(k)
        project(0, 0, 2 * rows, k)
        return 0

    lax.fori_loop(0, 2 * cuts, local_step, 0)

    def passed(s, j, h):
        ref = far_chunk(s, j, h)
        sem = cuts if s == 1 and j == 0 else j
        return copy_to(ref, ref, fwd_send.at[0], fwd_recv.at[sem], mate)

    def far_step(s, j):
        landed(far_chunk(s, j, core), link_recv.at[s, j])
        passed(s, j, core).start()
        project((2 + s) * rows, 2 * rows, rows, core * cuts + j)
        passed(s, j, other).wait_recv()
        project((2 + s) * rows, 2 * rows, rows, other * cuts + j)

    def part_copy(s, r):
        return copy_to(
            part.at[pl.ds((2 + s) * rows + r * step_rows, step_rows)],
            remote_in.at[pl.ds(r * step_rows, step_rows), cols(core * half, half)],
            rp_send.at[0],
            rp_recv.at[r],
            far + s,
        )

    def far_out(s):
        att_copy(2 + s, other).wait_recv()
        out_project(2 + s)
        for r in range(row_cuts):
            part_copy(s, r).start()

    for j in range(cuts):
        far_step(0, j)
    attend_slot(2 * rows, 2)
    att_copy(2, core).start()
    clear(2 * rows, rows)
    own_out.wait()
    landed(out_half.at[rws(other * q_cols, q_cols)], wo_sem.at[1])
    far_out(0)
    for j in range(cuts):
        far_step(1, j)
    attend_slot(2 * rows, 3)
    att_copy(3, core).start()
    far_out(1)
    attend_slot(0, 0)
    att_copy(0, core).start()
    attend_slot(rows, 1)
    att_copy(1, core).start()
    landed(attended.at[0 : 2 * rows, cols(other * q_cols, q_cols)], att_recv.at[0])
    out_project(other)
    near_copy = copy_to(
        part.at[rws(other * rows, rows)], local_in, lp_send, lp_recv, mate
    )
    near_copy.start()
    out_project(core)

    left(xbuf.at[rws(core * rows, rows)], x_send.at[0])
    push_out.wait_send()
    left(xbuf.at[0:rows, cols(core * half, half)], link_send.at[0])
    left(xbuf.at[0:rows, cols(core * half, half - chunk)], link_send.at[1])
    left(xbuf.at[0:keep_rows, cols(core * half, chunk)], link_send.at[2])

    @pl.when(core == 1)
    def _():
        left(xbuf.at[0 : rows - keep_rows, 0 : 2 * chunk], link_send.at[3])

    left(xbuf.at[2 * rows : 4 * rows, cols(core * half, half)], fwd_send.at[0])
    left(attended.at[:, cols(core * q_cols, q_cols)], att_send.at[0])
    near_copy.wait_send()
    near_copy.wait_recv()

    def finish(r, _):
        first = pl.multiple_of(r * step_rows, 16)
        at = pl.ds(first, step_rows)
        landed(remote_in.at[at], rp_recv.at[r])
        own_at, other_at = cols(core * half, half), cols(other * half, half)
        near = part[rws(core * rows + r * step_rows, step_rows)].astype(jnp.float32)
        a = near + remote_in[at, own_at].astype(jnp.float32)
        b = local_in[at].astype(jnp.float32) + remote_in[at, other_at].astype(jnp.float32)
        total = jnp.sum(a * a, axis=-1, keepdims=True) + jnp.sum(b * b, axis=-1, keepdims=True)
        scale = lax.rsqrt(total / width + norm_epsilon)
        mine = rws(core * rows + r * step_rows, step_rows)
        for piece, h in ((a, core), (b, other)):
            piece = piece * scale
            for i in range(half // 128):
                where = cols(h * half + i * 128, 128)
                gain = gain_post[pl.ds(h * (half // 128) + i, 1)]
                out[at, where] = (
                    xbuf[mine, where].astype(jnp.float32) + piece[:, i * 128 : (i + 1) * 128] * gain
                ).astype(jnp.bfloat16)
        return 0

    lax.fori_loop(0, row_cuts, finish, 0)
    left(part.at[2 * rows : 4 * rows], rp_send.at[0])


def fused(tokens, pre_gain, query_weight, key_weight, value_weight, out_weight, post_gain):
    rows, width = tokens.shape
    q_cols = query_weight.shape[1]
    k_cols = key_weight.shape[1]
    all_cols = q_cols + 2 * k_cols
    half = width // 2
    cuts = divisor(half // 128, 3)
    row_cuts = divisor(rows // 16, 8)
    head_rows = rows // 2
    keep_rows = rows // 2
    dma = pltpu.SemaphoreType.DMA
    bf16, f32 = jnp.bfloat16, jnp.float32
    return pl.pallas_call(
        functools.partial(fused_kernel, cuts, row_cuts, head_rows, keep_rows),
        out_shape=pltpu.VMEM((rows, width), bf16),
        in_specs=[pl.BlockSpec(memory_space=pl.ANY)] * 8,
        out_specs=pl.BlockSpec(memory_space=pltpu.VMEM),
        scratch_shapes=[
            pltpu.VMEM((4 * rows, width), bf16),
            pltpu.VMEM((2 * rows, half // cuts), bf16),
            pltpu.VMEM((3 * rows, all_cols), f32),
            pltpu.VMEM((3 * rows, 128), f32),
            pltpu.VMEM((width, all_cols), bf16),
            pltpu.VMEM((2 * q_cols, half), bf16),
            pltpu.VMEM((4 * rows, 2 * q_cols), bf16),
            pltpu.VMEM((4 * rows, half), bf16),
            pltpu.VMEM((rows, half), bf16),
            pltpu.VMEM((rows, width), bf16),
            pltpu.VMEM((width // 128, 128), f32),
            pltpu.VMEM((width // 128, 128), f32),
            pltpu.VMEM((2, SEQ_LEN, HEAD_DIM), f32),
            dma((4,)),
            dma((2 * cuts,)),
            dma((2,)),
            dma((1,)),
            dma((2,)),
            dma((4,)),
            dma((2, cuts)),
            dma((1,)),
            dma((cuts + 1,)),
            dma((1,)),
            dma((3,)),
            dma,
            dma,
            dma((1,)),
            dma((row_cuts,)),
        ],
        compiler_params=pltpu.CompilerParams(
            collective_id=0, has_side_effects=True, vmem_limit_bytes=63_000_000
        ),
    )(
        tokens,
        pre_gain.reshape(width // 128, 128),
        query_weight,
        key_weight,
        value_weight,
        out_weight,
        post_gain.reshape(width // 128, 128),
        jnp.asarray(rope_tables()),
    )


def body(tokens, *rest):
    rows, width = tokens.shape
    four = lax.axis_size("tensor") == 4
    if four and rows == SEQ_LEN and width % 768 == 0:
        return fused(tokens, *rest)
    return staged(tokens, *rest)


def solution(mesh):
    return jax.shard_map(
        body,
        mesh=mesh,
        in_specs=(
            P(("dp", "tensor"), None),
            P(),
            P(None, "tensor"),
            P(None, "tensor"),
            P(None, "tensor"),
            P("tensor", None),
            P(),
        ),
        out_specs=P(("dp", "tensor"), None),
        check_vma=False,
    )
```

```python
import functools

import jax
import jax.numpy as jnp
import numpy as np
from jax import lax
from jax.experimental import pallas as pl
from jax.experimental.pallas import tpu as pltpu
from jax.sharding import PartitionSpec as P

HEAD_DIM = 128
SEQ_LEN = 128


norm_epsilon = 1e-06
soft_cap = 50.0
query_scale = 1.0 / 12.0
rope_base = 10000.0


def rms_scale(vectors, scale_gain):
    mean_square = jnp.mean(vectors * vectors, axis=-1, keepdims=True)
    return vectors * lax.rsqrt(mean_square + norm_epsilon) * scale_gain


def rotate(vectors, positions):
    half_dim = vectors.shape[-1] // 2
    exponent = jnp.arange(half_dim, dtype=jnp.float32) / half_dim
    angles = positions.astype(jnp.float32)[:, None] * jnp.power(rope_base, -exponent)[None, :]
    cosine = jnp.cos(angles)[:, None, :]
    sine_part = jnp.sin(angles)[:, None, :]
    first_half = vectors[..., :half_dim]
    second_half = vectors[..., half_dim:]
    return jnp.concatenate(
        [
            first_half * cosine - second_half * sine_part,
            second_half * cosine + first_half * sine_part,
        ],
        axis=-1,
    )


def project_block(normed, query_weight, key_weight, value_weight):
    block_rows = normed.shape[0]
    positions = jnp.arange(block_rows, dtype=jnp.int32) % SEQ_LEN
    query = jnp.dot(normed, query_weight, preferred_element_type=jnp.float32)
    keys = jnp.dot(normed, key_weight, preferred_element_type=jnp.float32)
    values = jnp.dot(normed, value_weight, preferred_element_type=jnp.float32)
    query = rotate(query.reshape(block_rows, -1, HEAD_DIM), positions).reshape(block_rows, -1)
    keys = rotate(keys.reshape(block_rows, -1, HEAD_DIM), positions).reshape(block_rows, -1)
    return jnp.concatenate(
        [query.astype(jnp.bfloat16), keys.astype(jnp.bfloat16), values.astype(jnp.bfloat16)], axis=1
    )


def attend(query, keys, values, query_pos, key_pos):
    query_count = query.shape[0]
    key_count = keys.shape[0]
    key_heads = keys.shape[1] // HEAD_DIM
    groups = query.shape[1] // keys.shape[1]
    query_four = query.reshape(query_count, key_heads, groups, HEAD_DIM)
    key_three = keys.reshape(key_count, key_heads, HEAD_DIM)
    value_three = values.reshape(key_count, key_heads, HEAD_DIM)
    raw_scores = jnp.einsum(
        "qhgd,khd->hgqk", query_four, key_three, preferred_element_type=jnp.float32
    )
    capped = soft_cap * jnp.tanh(raw_scores * query_scale / soft_cap)
    allowed = jnp.logical_and(
        key_pos[None, :] <= query_pos[:, None],
        key_pos[None, :] // SEQ_LEN == query_pos[:, None] // SEQ_LEN,
    )
    weights = jnp.where(allowed[None, None], jnp.exp(capped), 0.0)
    probability = (weights / jnp.sum(weights, axis=-1, keepdims=True)).astype(jnp.bfloat16)
    mixed = jnp.einsum(
        "hgqk,khd->qhgd", probability, value_three, preferred_element_type=jnp.float32
    )
    return mixed.astype(jnp.bfloat16).reshape(query_count, -1)


def staged(tokens, pre_gain, query_weight, key_weight, value_weight, out_weight, post_gain):
    local_rows = tokens.shape[0]
    query_cols = query_weight.shape[1]
    key_cols = key_weight.shape[1]
    normed = rms_scale(tokens.astype(jnp.float32), pre_gain).astype(jnp.bfloat16)
    stacked = project_block(
        lax.all_gather(normed, "tensor", axis=0, tiled=True), query_weight, key_weight, value_weight
    )
    query = stacked[:, :query_cols]
    keys = stacked[:, query_cols : query_cols + key_cols]
    values = stacked[:, query_cols + key_cols :]
    token_count = stacked.shape[0]
    key_count = min(token_count, lax.axis_size("tensor") * local_rows + SEQ_LEN)
    key_first = jnp.clip(jnp.int32(0) // SEQ_LEN * SEQ_LEN, 0, token_count - key_count)
    query_pos = jnp.arange(lax.axis_size("tensor") * local_rows, dtype=jnp.int32)
    key_pos = key_first + jnp.arange(key_count, dtype=jnp.int32)
    block_out = attend(query, keys, values, query_pos, key_pos)
    mixed = lax.psum_scatter(
        jnp.dot(block_out, out_weight, preferred_element_type=jnp.float32).astype(jnp.bfloat16),
        "tensor",
        scatter_dimension=0,
        tiled=True,
    ).astype(jnp.float32)
    branch = rms_scale(mixed, post_gain)
    return (tokens.astype(jnp.float32) + branch).astype(jnp.bfloat16)


def rope_tables():
    half_dim = HEAD_DIM // 2
    angles = np.arange(SEQ_LEN)[:, None] * np.power(rope_base, -np.arange(half_dim) / half_dim)[None, :]
    cosine, sine = np.cos(angles), np.sin(angles)
    return np.stack(
        [np.concatenate([cosine, cosine], 1), np.concatenate([-sine, sine], 1)]
    ).astype(np.float32)


def divisor(count, wanted):
    return next(k for k in range(min(wanted, count), 0, -1) if count % k == 0)


def copy_to(src, dst, send_sem, recv_sem, index):
    return pltpu.make_async_remote_copy(
        src_ref=src,
        dst_ref=dst,
        send_sem=send_sem,
        recv_sem=recv_sem,
        device_id={"tensor": index},
        device_id_type=pl.DeviceIdType.MESH,
    )


def sent_rows(rows, width, q_cols, all_cols, chunk):
    half = width // 2
    total = rows * width + q_cols * half + 4 * rows * q_cols + 7 * rows * half - rows * chunk
    return total // all_cols if total % (16 * all_cols) == 0 else 0


def fused_kernel(
    cuts,
    pieces,
    head_rows,
    keep_rows,
    tokens,
    pre_gain,
    query_weight,
    key_weight,
    value_weight,
    out_weight,
    post_gain,
    rope_table,
    out,
    xbuf,
    scaled,
    acc,
    square,
    weight,
    out_half,
    attended,
    part,
    local_in,
    remote_in,
    gain_pre,
    gain_post,
    rope,
    in_sem,
    w_sem,
    sent,
    tail_sent,
    x_recv,
    out_recv,
    link_recv,
    fwd_recv,
    att_recv,
    rp_recv,
):
    rows, width = tokens.shape
    q_cols = query_weight.shape[1]
    k_cols = key_weight.shape[1]
    all_cols = q_cols + 2 * k_cols
    half = width // 2
    chunk = half // cuts
    groups = q_cols // k_cols
    kv_heads = k_cols // HEAD_DIM
    step_rows = 16
    n_tile = all_cols // divisor(all_cols // 128, 4)
    o_tile = half // divisor(half // 128, 3)

    me = lax.axis_index("tensor")
    core = me % 2
    other = 1 - core
    side = me // 2
    mate = side * 2 + other
    far = (1 - side) * 2

    def cols(start, size):
        return pl.ds(pl.multiple_of(start, 128), size)

    def rws(start, size):
        return pl.ds(pl.multiple_of(start, 16), size)

    def landed(ref, sem):
        copy_to(ref, ref, sem, sem, mate).wait_recv()

    def left(ref, sem):
        copy_to(ref, ref, sem, sem, mate).wait_send()

    own = pltpu.make_async_copy(tokens, xbuf.at[rws(core * rows, rows)], in_sem.at[0])
    own.start()
    small = [
        pltpu.make_async_copy(pre_gain, gain_pre, in_sem.at[1]),
        pltpu.make_async_copy(post_gain, gain_post, in_sem.at[1]),
        pltpu.make_async_copy(rope_table, rope, in_sem.at[1]),
    ]

    def weight_rows(k):
        return pl.ds(pl.multiple_of(k * chunk, 128), chunk)

    def weight_start(k):
        at = weight_rows(k)
        sem = w_sem.at[k // 2]
        pltpu.make_async_copy(query_weight.at[at], weight.at[at, 0:q_cols], sem).start()
        pltpu.make_async_copy(key_weight.at[at], weight.at[at, q_cols : q_cols + k_cols], sem).start()
        pltpu.make_async_copy(value_weight.at[at], weight.at[at, q_cols + k_cols : all_cols], sem).start()

    def weight_wait(k):
        ref = weight.at[pl.ds(pl.multiple_of(2 * k * chunk, 128), 2 * chunk)]
        pltpu.make_async_copy(ref, ref, w_sem.at[k]).wait()

    barrier = pltpu.get_barrier_semaphore()
    for index in (mate, far + core):
        pl.semaphore_signal(
            barrier, inc=1, device_id={"tensor": index}, device_id_type=pl.DeviceIdType.MESH
        )
    pl.semaphore_wait(barrier, 2)

    def x_copy(owner, h, sem):
        ref = xbuf.at[rws(owner * rows, rows), cols(h * half, half)]
        return copy_to(ref, ref, sent, x_recv.at[sem], mate)

    def far_chunk(s, j, h):
        return xbuf.at[pl.ds((2 + s) * rows, rows), cols(h * half + j * chunk, chunk)]

    def link_sem(s, j):
        return 2 * s + (j == cuts - 1)

    def link_at(s, j, h, first, last, sem=None, source=None):
        at = cols(h * half + j * chunk, chunk)
        if source is None:
            source = xbuf.at[pl.ds(s * rows + first, last - first), at]
        return copy_to(
            source,
            xbuf.at[pl.ds((2 + s) * rows + first, last - first), at],
            sent if sem is None else sem,
            link_recv.at[link_sem(s, j)],
            far + h,
        )

    def link_copy(s, j):
        first = head_rows if j == 0 else 0
        if s == 1 and j == cuts - 1:
            return link_at(s, j, core, first, keep_rows, tail_sent)
        return link_at(s, j, core, first, rows)

    def head_copy(s, source=None):
        return link_at(s, 0, core, 0, head_rows, source=source)

    def tail_copy(h):
        return link_at(1, cuts - 1, h, keep_rows, rows, tail_sent)

    @pl.when(core == 0)
    def _():
        head_copy(0, tokens.at[0:head_rows, cols(core * half, chunk)]).start()

    @pl.when(core == 1)
    def _():
        head_copy(1, tokens.at[0:head_rows, cols(core * half, chunk)]).start()

    for copy in small:
        copy.start()
    own.wait()
    x_copy(core, other, 0).start()

    @pl.when(core == 0)
    def _():
        for j in range(cuts):
            link_copy(0, j).start()

    x_copy(core, core, 1).start()

    def start_weights(k, _):
        weight_start(k)
        return 0

    lax.fori_loop(0, 2 * cuts, start_weights, 0)

    x_copy(other, core, 0).wait_recv()

    @pl.when(core == 1)
    def _():
        head_copy(0).start()
        for j in range(cuts):
            link_copy(0, j).start()
        for j in range(cuts - 1):
            link_copy(1, j).start()
        link_copy(1, cuts - 1).start()
        tail_copy(1).start()

    @pl.when(core == 0)
    def _():
        head_copy(1).start()
        for j in range(cuts):
            link_copy(1, j).start()

    own_out = pltpu.make_async_copy(
        out_weight.at[:, cols(core * half, half)],
        out_half.at[rws(core * q_cols, q_cols)],
        in_sem.at[0],
    )
    own_out.start()
    push_out = copy_to(
        out_weight.at[:, cols(other * half, half)],
        out_half.at[rws(core * q_cols, q_cols)],
        sent,
        out_recv,
        mate,
    )
    push_out.start()
    x_copy(other, other, 1).wait_recv()
    small_ref = acc.at[0 : 2 * gain_pre.shape[0] + 2 * SEQ_LEN, 0:128]
    pltpu.make_async_copy(small_ref, small_ref, in_sem.at[1]).wait()

    def project(first_row, acc_row, count, k):
        ar = pl.ds(acc_row, count)
        at = cols(k * chunk, chunk)
        total = square[ar]
        for i in range(chunk // 128):
            x = xbuf[pl.ds(first_row, count), cols(k * chunk + i * 128, 128)].astype(jnp.float32)
            total = total + x * x
            gain = gain_pre[pl.ds(k * (chunk // 128) + i, 1)]
            scaled[0:count, i * 128 : (i + 1) * 128] = (x * gain).astype(jnp.bfloat16)
        square[ar] = total

        def tile(n, _):
            nat = cols(n * n_tile, n_tile)
            acc[ar, nat] += jnp.dot(
                scaled[0:count], weight[at, nat], preferred_element_type=jnp.float32
            )
            return 0

        lax.fori_loop(0, all_cols // n_tile, tile, 0, unroll=True)

    def clear(row, count):
        acc[pl.ds(row, count)] = jnp.zeros((count, all_cols), jnp.float32)
        square[pl.ds(row, count)] = jnp.zeros((count, 128), jnp.float32)

    def attend_slot(acc_row, slot):
        ar = rws(acc_row, rows)
        scale = lax.rsqrt(
            jnp.sum(square[ar], axis=-1, keepdims=True) / width + norm_epsilon
        )
        cosine, sine = rope[0], rope[1]
        ok = lax.broadcasted_iota(jnp.int32, (rows, rows), 1) <= lax.broadcasted_iota(
            jnp.int32, (rows, rows), 0
        )
        ok = jnp.concatenate([ok] * groups, axis=0)

        def turned(at):
            v = acc[ar, at] * scale
            return (v * cosine + pltpu.roll(v, HEAD_DIM // 2, 1) * sine).astype(jnp.bfloat16)

        def head(g, _):
            query = jnp.concatenate(
                [turned(cols((g * groups + i) * HEAD_DIM, HEAD_DIM)) for i in range(groups)], axis=0
            )
            keys = turned(cols(q_cols + g * HEAD_DIM, HEAD_DIM))
            values = (acc[ar, cols(q_cols + k_cols + g * HEAD_DIM, HEAD_DIM)] * scale).astype(jnp.bfloat16)
            raw = lax.dot_general(
                query, keys, (((1,), (1,)), ((), ())), preferred_element_type=jnp.float32
            )
            capped = soft_cap * jnp.tanh(raw * (query_scale / soft_cap))
            mass = jnp.where(ok, jnp.exp(capped), 0.0)
            prob = (mass / jnp.sum(mass, axis=-1, keepdims=True)).astype(jnp.bfloat16)
            mixed = jnp.dot(prob, values, preferred_element_type=jnp.float32).astype(jnp.bfloat16)
            for i in range(groups):
                attended[
                    rws(slot * rows, rows), cols(core * q_cols + (g * groups + i) * HEAD_DIM, HEAD_DIM)
                ] = mixed[i * rows : (i + 1) * rows]
            return 0

        lax.fori_loop(0, kv_heads, head, 0)

    def att_copy(slot, whose):
        ref = attended.at[pl.ds(slot * rows, rows), cols(whose * q_cols, q_cols)]
        return copy_to(ref, ref, sent, att_recv.at[int(slot == 3)], mate)

    def out_project(slot):
        def tile(n, _):
            at = cols(n * o_tile, o_tile)
            part[rws(slot * rows, rows), at] = jnp.dot(
                attended[rws(slot * rows, rows)], out_half[:, at], preferred_element_type=jnp.float32
            ).astype(jnp.bfloat16)
            return 0

        lax.fori_loop(0, half // o_tile, tile, 0, unroll=True)

    clear(0, 3 * rows)

    def local_step(k, _):
        weight_wait(k)
        for i in range(2):
            project(0, 0, 2 * rows, 2 * k + i)
        return 0

    lax.fori_loop(0, cuts, local_step, 0)

    def far_cols(s, last, h):
        first = cuts - 1 if last else 0
        count = 1 if last else cuts - 1
        return xbuf.at[
            pl.ds((2 + s) * rows, rows), cols(h * half + first * chunk, count * chunk)
        ]

    def passed(s, last, h):
        ref = far_cols(s, last, h)
        return copy_to(ref, ref, sent, fwd_recv.at[2 * s + last], mate)

    def far_step(s, last):
        landed(far_cols(s, last, core), link_recv.at[2 * s + last])
        if s == 0 and not last:

            @pl.when(core == 1)
            def _():
                tail_copy(0).start()

        passed(s, last, core).start()
        which = range(cuts - 1, cuts) if last else range(cuts - 1)
        for j in which:
            project((2 + s) * rows, 2 * rows, rows, core * cuts + j)
        passed(s, last, other).wait_recv()
        for j in which:
            project((2 + s) * rows, 2 * rows, rows, other * cuts + j)

    def part_copy(s, p):
        at = pl.ds(sum(pieces[:p]), pieces[p])
        return copy_to(
            part.at[pl.ds((2 + s) * rows + sum(pieces[:p]), pieces[p])],
            remote_in.at[at, cols(core * half, half)],
            sent,
            rp_recv.at[p],
            far + s,
        )

    def far_out(s):
        att_copy(2 + s, other).wait_recv()
        out_project(2 + s)
        for p in range(len(pieces)):
            part_copy(s, p).start()

    for last in range(2):
        far_step(0, last)
    attend_slot(2 * rows, 2)
    att_copy(2, core).start()
    clear(2 * rows, rows)
    own_out.wait()
    landed(out_half.at[rws(other * q_cols, q_cols)], out_recv)
    far_out(0)
    for last in range(2):
        far_step(1, last)
    attend_slot(2 * rows, 3)
    att_copy(3, core).start()
    far_out(1)
    attend_slot(0, 0)
    att_copy(0, core).start()
    attend_slot(rows, 1)
    att_copy(1, core).start()
    landed(attended.at[0 : 2 * rows, cols(other * q_cols, q_cols)], att_recv.at[0])
    out_project(other)
    near_copy = copy_to(
        part.at[rws(other * rows, rows)], local_in, sent, out_recv, mate
    )
    near_copy.start()
    out_project(core)

    near_copy.wait_recv()

    def finish(r, _):
        first = pl.multiple_of(r * step_rows, 16)
        at = pl.ds(first, step_rows)
        own_at, other_at = cols(core * half, half), cols(other * half, half)
        near = part[rws(core * rows + r * step_rows, step_rows)].astype(jnp.float32)
        a = near + remote_in[at, own_at].astype(jnp.float32)
        b = local_in[at].astype(jnp.float32) + remote_in[at, other_at].astype(jnp.float32)
        total = jnp.sum(a * a, axis=-1, keepdims=True) + jnp.sum(b * b, axis=-1, keepdims=True)
        scale = lax.rsqrt(total / width + norm_epsilon)
        mine = rws(core * rows + r * step_rows, step_rows)
        for piece, h in ((a, core), (b, other)):
            piece = piece * scale
            for i in range(half // 128):
                where = cols(h * half + i * 128, 128)
                gain = gain_post[pl.ds(h * (half // 128) + i, 1)]
                out[at, where] = (
                    xbuf[mine, where].astype(jnp.float32) + piece[:, i * 128 : (i + 1) * 128] * gain
                ).astype(jnp.bfloat16)
        return 0

    for p, count in enumerate(pieces):
        first = sum(pieces[:p])
        landed(remote_in.at[pl.ds(first, count)], rp_recv.at[p])
        lax.fori_loop(first // step_rows, (first + count) // step_rows, finish, 0)

    left(weight.at[0 : sent_rows(rows, width, q_cols, all_cols, chunk)], sent)

    @pl.when(core == 0)
    def _():
        left(xbuf.at[0:keep_rows, 0:chunk], tail_sent)

    @pl.when(core == 1)
    def _():
        left(xbuf.at[0 : 2 * rows - keep_rows, 0:chunk], tail_sent)


def fused(tokens, pre_gain, query_weight, key_weight, value_weight, out_weight, post_gain):
    rows, width = tokens.shape
    q_cols = query_weight.shape[1]
    k_cols = key_weight.shape[1]
    all_cols = q_cols + 2 * k_cols
    half = width // 2
    cuts = 3
    pieces = (3 * rows // 8, 3 * rows // 8, rows // 8, rows // 8)
    head_rows = rows // 2
    keep_rows = rows // 2
    dma = pltpu.SemaphoreType.DMA
    bf16, f32 = jnp.bfloat16, jnp.float32
    return pl.pallas_call(
        functools.partial(fused_kernel, cuts, pieces, head_rows, keep_rows),
        out_shape=pltpu.VMEM((rows, width), bf16),
        in_specs=[pl.BlockSpec(memory_space=pl.ANY)] * 8,
        out_specs=pl.BlockSpec(memory_space=pltpu.VMEM),
        scratch_shapes=[
            pltpu.VMEM((4 * rows, width), bf16),
            pltpu.VMEM((2 * rows, half // cuts), bf16),
            pltpu.VMEM((3 * rows, all_cols), f32),
            pltpu.VMEM((3 * rows, 128), f32),
            pltpu.VMEM((width, all_cols), bf16),
            pltpu.VMEM((2 * q_cols, half), bf16),
            pltpu.VMEM((4 * rows, 2 * q_cols), bf16),
            pltpu.VMEM((4 * rows, half), bf16),
            pltpu.VMEM((rows, half), bf16),
            pltpu.VMEM((rows, width), bf16),
            pltpu.VMEM((width // 128, 128), f32),
            pltpu.VMEM((width // 128, 128), f32),
            pltpu.VMEM((2, SEQ_LEN, HEAD_DIM), f32),
            dma((2,)),
            dma((cuts,)),
            dma,
            dma,
            dma((2,)),
            dma,
            dma((4,)),
            dma((4,)),
            dma((2,)),
            dma((len(pieces),)),
        ],
        compiler_params=pltpu.CompilerParams(
            collective_id=0, has_side_effects=True, vmem_limit_bytes=63_000_000
        ),
    )(
        tokens,
        pre_gain.reshape(width // 128, 128),
        query_weight,
        key_weight,
        value_weight,
        out_weight,
        post_gain.reshape(width // 128, 128),
        jnp.asarray(rope_tables()),
    )


def body(tokens, *rest):
    rows, width = tokens.shape
    q_cols, all_cols = rest[1].shape[1], sum(w.shape[1] for w in rest[1:4])
    four = lax.axis_size("tensor") == 4
    if four and rows == SEQ_LEN and width % 768 == 0:
        if sent_rows(rows, width, q_cols, all_cols, width // 6):
            return fused(tokens, *rest)
    return staged(tokens, *rest)


def solution(mesh):
    return jax.shard_map(
        body,
        mesh=mesh,
        in_specs=(
            P(("dp", "tensor"), None),
            P(),
            P(None, "tensor"),
            P(None, "tensor"),
            P(None, "tensor"),
            P("tensor", None),
            P(),
        ),
        out_specs=P(("dp", "tensor"), None),
        check_vma=False,
    )
```
